512 devices in a mesh: grid: 64 (over y, z), freq: 8 (over x, core).
Axes of the slice: x: 4, y: 8, z: 8, core: 2. Of those that a mesh axis runs over, the one named last changes fastest.
Arguments:
- replicas: bfloat16 [16, 32768, 2, 512], P('freq', 'grid'), may hold values from -6 to 6
- csm: bfloat16 [16, 2, 512, 512], P('freq', None, 'grid'), as said below
- inverse: bfloat16 [16, 2, 512, 512], P('freq', None, 'grid'), as said below
Outputs:
- bartlett: float32 [32768], P(('grid', 'freq'))
- mvdr: float32 [32768], P(('grid', 'freq'))
The draws below stay inside these ranges and needn't reach their ends.
Inputs may be any that keep to these rules, and one draw needn't show every extreme that they name: csm[f, 0] + i csm[f, 1] is Hermitian positive definite for every bin. inverse[f, 0] + i inverse[f, 1] is Hermitian positive definite for every bin.
All inputs are finite; a program needn't handle non-finite values.
Results may differ from the reference program's by a relative error of at most 0.0003.
Values may be sent and summed in bfloat16 or wider, within the bound.
No kernel may reach another device: no remote copies, remote signals or barrier semaphores. Data moves between devices by JAX's collectives and lax.ppermute only.
A program may use at most 64 MiB of HBM per device.

```python
import jax
import jax.numpy as jnp
from jax import lax

M = 512
F = 16
G = 32768


def hermitian(key):
    first, second, third, fourth = jax.random.split(key, 4)
    real_part = jax.random.normal(first, (F, M, M), jnp.float32)
    imag_part = jax.random.normal(second, (F, M, M), jnp.float32)
    outer_rr = jnp.einsum('fik,fjk->fij', real_part, real_part, precision=lax.Precision.HIGHEST)
    outer_ii = jnp.einsum('fik,fjk->fij', imag_part, imag_part, precision=lax.Precision.HIGHEST)
    outer_ir = jnp.einsum('fik,fjk->fij', imag_part, real_part, precision=lax.Precision.HIGHEST)
    gram_real = (outer_rr + outer_ii) / M
    gram_imag = (outer_ir - jnp.swapaxes(outer_ir, 1, 2)) / M
    loading = jax.random.uniform(third, (F, M), jnp.float32, 1.0, 2.0)
    scales = jnp.exp(jax.random.uniform(fourth, (F, M), jnp.float32, 0.0, jnp.log(4.0)))
    gram_real = gram_real + jnp.eye(M, dtype=jnp.float32)[None] * loading[:, :, None]
    outer_scale = scales[:, :, None] * scales[:, None, :]
    return jnp.stack([gram_real * outer_scale, gram_imag * outer_scale], axis=1)


def draw_csm(key, part):
    return hermitian(jax.random.fold_in(key, 11)).astype(jnp.bfloat16)


def draw_inverse(key, part):
    return hermitian(jax.random.fold_in(key, 23)).astype(jnp.bfloat16)


def block_scale(key, dims, shards, least, high):
    level = 1.0
    for axis_at, blocks in shards:
        heights = jax.random.uniform(jax.random.fold_in(jax.random.fold_in(key, 6), axis_at), (blocks,), jnp.float32, least / len(shards), high / len(shards))
        level = level * jnp.repeat(jnp.exp(heights), dims[axis_at] // blocks).reshape((-1,) + (1,) * (len(dims) - 1 - axis_at))
    return level


def bell_draw(stream_key, shape, deviation, most, pieces=(), kind=jnp.bfloat16):
    drawn = jax.random.normal(stream_key, shape, jnp.float32) * deviation
    if len(pieces) > 0:
        drawn = block_scale(stream_key, shape, pieces, -0.22, 0.18) * drawn
    return jnp.clip(drawn, min=-most, max=most).astype(kind)


def setup_inputs(seed: int = 0) -> dict:
    splits = jax.random.split(jax.random.key(seed), 4)
    return {
        "replicas": bell_draw(splits[0], (F, G, 2, M), 1.0, 6.0, ((0, 8), (1, 64))),
        "csm": draw_csm(jax.random.fold_in(splits[3], 71), 0),
        "inverse": draw_inverse(jax.random.fold_in(splits[3], 71), 0),
    }


def stacked(mat):
    real = mat[0].astype(jnp.float32)
    imag = mat[1].astype(jnp.float32)
    upper = jnp.concatenate([real, -imag], axis=1)
    lower = jnp.concatenate([imag, real], axis=1)
    return jnp.concatenate([upper, lower], axis=0)


def one_bin(inputs):
    vectors, matrix, inverted = inputs
    count = vectors.shape[0]
    wide = vectors.reshape(count, 2 * vectors.shape[2]).astype(jnp.float32)
    energy = jnp.sum(wide * wide, axis=1) + 1e-6
    power = jnp.sum(jnp.dot(wide, stacked(matrix), precision=lax.Precision.HIGHEST) * wide, axis=1)
    quad = jnp.sum(jnp.dot(wide, stacked(inverted), precision=lax.Precision.HIGHEST) * wide, axis=1)
    single_b = power / energy
    single_m = energy / quad
    return single_b / jnp.max(single_b), single_m / jnp.max(single_m)


def reference(replicas, csm, inverse):
    surf_b, surf_m = lax.map(one_bin, (replicas, csm, inverse))
    bins = replicas.shape[0]
    return jnp.sum(surf_b, axis=0) / bins, jnp.sum(surf_m, axis=0) / bins
```

```python
import functools

import jax
import jax.numpy as jnp
import numpy as np
from jax import lax
from jax.experimental import pallas as pl
from jax.experimental.layout import Layout, with_layout_constraint
from jax.experimental.pallas import tpu as pltpu
from jax.sharding import Mesh
from jax.sharding import PartitionSpec as P

ALL = ("yh", "yl", "zh", "zl", "x", "c")
MIB = 1 << 20


def device_ids(shape):
    return np.arange(np.prod(shape)).reshape(shape)


def lines(shape, first):
    ids = device_ids(shape)
    by_y = np.moveaxis(ids, 0, -1)
    by_z = np.moveaxis(ids, 1, -1)
    pair = (by_z, by_y) if first else (by_y, by_z)
    picked = [part[..., core, :].reshape(-1, part.shape[-1]) for core, part in enumerate(pair)]
    return np.concatenate(picked, axis=0).tolist()


def partners(shape):
    ids = device_ids(shape)
    pairs = []
    for core in range(shape[3]):
        plane = ids[..., core]
        other = plane[np.arange(shape[0]) ^ 1] if core == 0 else plane[:, np.arange(shape[1]) ^ 1]
        pairs += zip(plane.ravel().tolist(), other.ravel().tolist())
    return pairs


def role():
    return jnp.where(lax.axis_index("c") == 0, lax.axis_index("yl"), lax.axis_index("zl"))


def pack_kernel(n_z, csm_hbm, inverse_hbm, held_hbm, rows_hbm, given_hbm, matrices, packed, room, sems):
    bins, _, depth, width = csm_hbm.shape
    to_all, (parts, size) = rows_hbm.shape[0], room.shape[:2]
    chosen = 1 - role()
    reads = [pltpu.make_async_copy(ref, matrices.at[k], sems.at[k]) for k, ref in enumerate((csm_hbm, inverse_hbm))]
    at = len(reads)
    takes = [
        pltpu.make_async_copy(held_hbm.at[chosen, pl.ds(k * size, size)], room.at[k], sems.at[at + k])
        for k in range(parts)
    ]
    at += parts
    gives = [
        pltpu.make_async_copy(room.at[k], given_hbm.at[pl.ds(k * size, size)], sems.at[at + k]) for k in range(parts)
    ]
    at += parts
    sends = [pltpu.make_async_copy(packed, rows_hbm.at[to], sems.at[at + to]) for to in range(to_all)]
    for copy in reads + takes:
        copy.start()
    y = lax.axis_index("yh") * 2 + lax.axis_index("yl")
    z = lax.axis_index("zh") * 2 + lax.axis_index("zl")
    start = (y * n_z + z) * depth
    row = start + lax.broadcasted_iota(jnp.int32, (depth, width), 0)
    col = lax.broadcasted_iota(jnp.int32, (depth, width), 1)
    weight = jnp.where(col == row, 0.5, 1.0)
    for copy in reads:
        copy.wait()
    for b in range(bins):
        for m in range(2):
            real = matrices[m, b, 0].astype(jnp.float32) * weight
            imag = matrices[m, b, 1].astype(jnp.float32)
            packed[b, m] = jnp.where(col >= row, real, imag).astype(packed.dtype)
    for take, give in zip(takes, gives):
        take.wait()
        give.start()
    for copy in sends:
        copy.start()
    for copy in sends + gives:
        copy.wait()


def pack(n_z, csm, inverse, held, parts=4):
    bins, _, depth, width = csm.shape
    _, points, two, _ = held.shape
    hbm = pl.BlockSpec(memory_space=pltpu.HBM)
    return pl.pallas_call(
        functools.partial(pack_kernel, n_z),
        out_shape=(
            jax.ShapeDtypeStruct((n_z, bins, 2, depth, width), csm.dtype),
            jax.ShapeDtypeStruct(held.shape[1:], held.dtype),
        ),
        in_specs=[hbm] * 3,
        out_specs=[hbm] * 2,
        scratch_shapes=[
            pltpu.VMEM((2, *csm.shape), csm.dtype),
            pltpu.VMEM((bins, 2, depth, width), csm.dtype),
            pltpu.VMEM((parts, points // parts, two, width), held.dtype),
            pltpu.SemaphoreType.DMA((2 + 2 * parts + n_z,)),
        ],
        cost_estimate=pl.CostEstimate(flops=0, bytes_accessed=2 * held.size, transcendentals=0),
        compiler_params=pltpu.CompilerParams(vmem_limit_bytes=61 * MIB),
        name="pack",
    )(csm, inverse, held)


def forms_kernel(rows_ref, own_ref, other_ref, e_own_ref, e_other_ref, out_ref, mat_ref):
    n_y, n_z, _, depth, width = rows_ref.shape
    half = width // 2
    core = lax.axis_index("c")
    swapped = core == 1

    for m in range(2):
        for at in range(n_y * n_z):
            y, z = at // n_z, at % n_z
            first, second = jnp.where(swapped, z, y), jnp.where(swapped, y, z)
            mat_ref[m, at * depth : (at + 1) * depth, :] = rows_ref[first, second, m]
    row = lax.broadcasted_iota(jnp.int32, (half, half), 0)
    col = lax.broadcasted_iota(jnp.int32, (half, half), 1)
    upper = col >= row
    zero = jnp.zeros((half, half), mat_ref.dtype)
    dot = functools.partial(jnp.dot, preferred_element_type=jnp.float32)
    lanes = lambda *parts: jnp.concatenate(parts, axis=1)
    tall = lambda *parts: jnp.concatenate(parts, axis=0)
    wide = lambda value: value.astype(jnp.float32)
    blocks = []
    for m in range(2):
        m00 = mat_ref[m, :half, :half]
        m11 = mat_ref[m, half:, half:]
        u01 = mat_ref[m, :half, half:]
        l10 = mat_ref[m, half:, :half]
        u00, l00 = jnp.where(upper, m00, zero), jnp.where(upper, zero, m00)
        u11, l11 = jnp.where(upper, m11, zero), jnp.where(upper, zero, m11)
        blocks.append(
            (lanes(u00, u01, -l00), lanes(l00, u00, u01), lanes(u11, -l10, -l11), lanes(l10, l11, u11))
        )
    stacked = [tall(*pair) for pair in zip(*blocks)]
    singles, peaks = [], [None, None]
    for wave_ref, energy_ref in ((own_ref, e_own_ref), (other_ref, e_other_ref)):
        r0, r1 = wave_ref[0, :half], wave_ref[0, half:]
        i0, i1 = wave_ref[1, :half], wave_ref[1, half:]
        totals = [None, None]
        for left, right, times in zip(
            stacked,
            (tall(r0, r1, i0), tall(r0, i0, i1), tall(r1, i0, i1), tall(r0, r1, i1)),
            (r0, i0, r1, i1),
        ):
            image = dot(left, right)
            times = wide(times)
            for m in range(2):
                part = jnp.sum(image[m * half : (m + 1) * half] * times, axis=0)
                totals[m] = part if totals[m] is None else totals[m] + part
        energy = energy_ref[...]
        power, quad = 2.0 * totals[0][None], 2.0 * totals[1][None]
        single = (power / energy, energy / quad)
        singles.append(single)
        for m in range(2):
            top = jnp.max(single[m], axis=1, keepdims=True)
            peaks[m] = top if peaks[m] is None else jnp.maximum(peaks[m], top)
    part_of = role()
    lane = lax.broadcasted_iota(jnp.int32, (1, 128), 1)
    at = ((lax.axis_index("x") * 2 + core) * 2 + part_of) * 2
    mark = jnp.where(lane == at, peaks[0], jnp.where(lane == at + 1, peaks[1], -jnp.inf))
    n_f = out_ref.shape[0] // 4
    share = own_ref.shape[2] // n_f
    for f in range(n_f):
        own, other = (lanes(*(p[:, f * share : (f + 1) * share] for p in single)) for single in singles)
        for py in range(2):
            for pz in range(2):
                mine = jnp.where(core == 0, py, pz) == part_of
                out_ref[(py * 2 + pz) * n_f + f] = lanes(jnp.where(mine, own, other), mark)


def fan_kernel(near_ref, out_hbm, sems):
    bins = near_ref.shape[1]
    sends = [
        pltpu.make_async_copy(near_ref.at[:, to % bins], out_hbm.at[to], sems.at[to]) for to in range(out_hbm.shape[0])
    ]
    for copy in sends:
        copy.start()
    for copy in sends:
        copy.wait()


def fan(near, n_y):
    n_z, _, *rest = near.shape
    return pl.pallas_call(
        fan_kernel,
        out_shape=jax.ShapeDtypeStruct((n_y, n_z, *rest), near.dtype),
        in_specs=[pl.BlockSpec(memory_space=pltpu.VMEM)],
        out_specs=pl.BlockSpec(memory_space=pltpu.HBM),
        scratch_shapes=[pltpu.SemaphoreType.DMA((n_y,))],
        cost_estimate=pl.CostEstimate(flops=0, bytes_accessed=10 * near.size, transcendentals=0),
        compiler_params=pltpu.CompilerParams(vmem_limit_bytes=4 * MIB),
        name="fan",
    )(near)


def peaks_kernel(parts_ref, out_ref):
    width = out_ref.shape[2]
    top = parts_ref[0, :, width:]
    for source in range(1, parts_ref.shape[0]):
        top = jnp.maximum(top, parts_ref[source, :, width:])
    for to in range(out_ref.shape[0]):
        out_ref[to] = top


def total_kernel(count, parts_ref, tops_ref, first_ref, second_ref):
    odd_y, odd_z = lax.axis_index("yl") == 1, lax.axis_index("zl") == 1
    n_f = parts_ref.shape[0] // 4
    width = tops_ref.shape[2]
    share = width // 2
    top = tops_ref[0]
    for source in range(1, tops_ref.shape[0]):
        top = jnp.maximum(top, tops_ref[source])
    lane = lax.broadcasted_iota(jnp.int32, (1, width), 1)
    total = jnp.zeros((1, width), jnp.float32)
    for f in range(n_f):
        for part_of in range(2):
            low = part_of * 2 * n_f + f if f % 2 == 0 else part_of * n_f + f
            high = low + (n_f if f % 2 == 0 else 2 * n_f)
            odd = odd_z if f % 2 == 0 else odd_y
            part = jnp.where(odd, parts_ref[high, :, :width], parts_ref[low, :, :width])
            at = (f * 2 + part_of) * 2
            total += part / jnp.where(lane < share, top[:, at : at + 1], top[:, at + 1 : at + 2])
    total = total * (1.0 / count)
    first_ref[...] = total[:, :share]
    second_ref[...] = total[:, share:]


def kernel_call(kernel, outs, operands, scratch=(), limit=4 * MIB, flops=0, dtype=jnp.float32):
    vmem = pl.BlockSpec(memory_space=pltpu.VMEM)
    cost = pl.CostEstimate(flops=flops, bytes_accessed=sum(a.size for a in operands), transcendentals=0)
    return pl.pallas_call(
        kernel,
        out_shape=tuple(jax.ShapeDtypeStruct(s, dtype) for s in outs),
        in_specs=[vmem] * len(operands),
        out_specs=[vmem] * len(outs),
        scratch_shapes=list(scratch),
        cost_estimate=cost,
        compiler_params=pltpu.CompilerParams(vmem_limit_bytes=limit),
    )(*operands)


def body(shape, replicas, csm, inverse):
    n_y, n_z, n_x, n_c = shape
    bins, points, _, width = replicas.shape
    natural = Layout(major_to_minor=(0, 1, 2))
    rows, given = pack(n_z, csm, inverse, replicas)
    got = lax.ppermute(with_layout_constraint(given, natural), ALL, partners(shape))
    got = with_layout_constraint(got, natural)
    kept = lax.dynamic_index_in_dim(replicas, role(), 0, keepdims=False)

    near = lax.all_to_all(rows, ALL, 0, 0, axis_index_groups=lines(shape, True), tiled=True)
    both = lax.all_to_all(fan(near, n_y), ALL, 0, 0, axis_index_groups=lines(shape, False), tiled=True)

    waves, energies = [], []
    for held in (kept, got):
        waves.append(jnp.transpose(held, (1, 2, 0)))
        wide = held.astype(jnp.float32)
        energies.append((jnp.sum(wide * wide, axis=(1, 2)) + 1e-06)[None])
    n_f = n_x * n_c
    share = points // n_f
    (parts,) = kernel_call(
        forms_kernel,
        ((4 * n_f, 1, 2 * share + 128),),
        (both, *waves, *energies),
        scratch=[pltpu.VMEM((2, width, width), jnp.bfloat16)],
        limit=24 * MIB,
        flops=2 * 2 * 12 * 2 * (width // 2) ** 2 * points,
    )
    parts = lax.all_to_all(parts, ("yl", "zl", "x", "c"), 0, 0, tiled=True)
    (tops,) = kernel_call(peaks_kernel, ((n_y * n_z // 4, 1, 128),), (parts,))
    tops = lax.all_to_all(tops, ("yh", "zh"), 0, 0, tiled=True)
    total = functools.partial(total_kernel, bins * n_f)
    first, second = kernel_call(total, ((1, share), (1, share)), (parts, tops))
    return first[0], second[0]


def solution(mesh):
    side = round(mesh.shape["grid"] ** 0.5)
    shape = (side, side, mesh.shape["freq"] // 2, 2)
    fine = Mesh(mesh.devices.reshape(side // 2, 2, side // 2, 2, *shape[2:]), ALL)
    grid, freq = ALL[:4], ALL[4:]
    in_specs = (P(freq, grid, None, None), P(freq, None, grid, None), P(freq, None, grid, None))
    out_specs = (P(ALL), P(ALL))

    def run(*inputs):
        return body(shape, *inputs)

    return jax.shard_map(run, mesh=fine, in_specs=in_specs, out_specs=out_specs, check_vma=False)
```

```python
import functools

import jax
import jax.numpy as jnp
import numpy as np
from jax import lax
from jax.experimental import pallas as pl
from jax.experimental.layout import Layout, with_layout_constraint
from jax.experimental.pallas import tpu as pltpu
from jax.sharding import Mesh
from jax.sharding import PartitionSpec as P

ALL = ("yh", "yl", "zh", "zl", "x", "c")
MIB = 1 << 20


def device_ids(shape):
    return np.arange(np.prod(shape)).reshape(shape)


def lines(shape, first):
    ids = device_ids(shape)
    by_y = np.moveaxis(ids, 0, -1)
    by_z = np.moveaxis(ids, 1, -1)
    pair = (by_z, by_y) if first else (by_y, by_z)
    picked = [part[..., core, :].reshape(-1, part.shape[-1]) for core, part in enumerate(pair)]
    return np.concatenate(picked, axis=0).tolist()


def partners(shape):
    ids = device_ids(shape)
    pairs = []
    for core in range(shape[3]):
        plane = ids[..., core]
        other = plane[:, np.arange(shape[1]) ^ 1] if core == 0 else plane[np.arange(shape[0]) ^ 1]
        pairs += zip(plane.ravel().tolist(), other.ravel().tolist())
    return pairs


def role():
    return jnp.where(lax.axis_index("c") == 0, lax.axis_index("zl"), lax.axis_index("yl"))


def pack_kernel(n_z, csm_hbm, inverse_hbm, held_hbm, rows_hbm, given_hbm, matrices, packed, room, sems):
    bins, _, depth, width = csm_hbm.shape
    to_all, (parts, size) = rows_hbm.shape[0], room.shape[:2]
    chosen = 1 - role()
    reads = [pltpu.make_async_copy(ref, matrices.at[k], sems.at[k]) for k, ref in enumerate((csm_hbm, inverse_hbm))]
    at = len(reads)
    takes = [
        pltpu.make_async_copy(held_hbm.at[chosen, pl.ds(k * size, size)], room.at[k], sems.at[at + k])
        for k in range(parts)
    ]
    at += parts
    gives = [
        pltpu.make_async_copy(room.at[k], given_hbm.at[pl.ds(k * size, size)], sems.at[at + k]) for k in range(parts)
    ]
    at += parts
    sends = [pltpu.make_async_copy(packed.at[to % bins], rows_hbm.at[to], sems.at[at + to]) for to in range(to_all)]
    for copy in reads + takes:
        copy.start()
    y = lax.axis_index("yh") * 2 + lax.axis_index("yl")
    z = lax.axis_index("zh") * 2 + lax.axis_index("zl")
    start = (y * n_z + z) * depth
    row = start + lax.broadcasted_iota(jnp.int32, (depth, width), 0)
    col = lax.broadcasted_iota(jnp.int32, (depth, width), 1)
    weight = jnp.where(col == row, 0.5, 1.0)
    for copy in reads:
        copy.wait()
    for b in range(bins):
        for m in range(2):
            real = matrices[m, b, 0].astype(jnp.float32) * weight
            imag = matrices[m, b, 1].astype(jnp.float32)
            packed[b, m] = jnp.where(col >= row, real, imag).astype(packed.dtype)
    for take, give in zip(takes, gives):
        take.wait()
        give.start()
    for copy in sends:
        copy.start()
    for copy in sends + gives:
        copy.wait()


def pack(n_z, csm, inverse, held, parts=4):
    bins, _, depth, width = csm.shape
    _, points, two, _ = held.shape
    hbm = pl.BlockSpec(memory_space=pltpu.HBM)
    return pl.pallas_call(
        functools.partial(pack_kernel, n_z),
        out_shape=(
            jax.ShapeDtypeStruct((n_z, 2, depth, width), csm.dtype),
            jax.ShapeDtypeStruct(held.shape[1:], held.dtype),
        ),
        in_specs=[hbm] * 3,
        out_specs=[hbm] * 2,
        scratch_shapes=[
            pltpu.VMEM((2, *csm.shape), csm.dtype),
            pltpu.VMEM((bins, 2, depth, width), csm.dtype),
            pltpu.VMEM((parts, points // parts, two, width), held.dtype),
            pltpu.SemaphoreType.DMA((2 + 2 * parts + n_z,)),
        ],
        cost_estimate=pl.CostEstimate(flops=0, bytes_accessed=2 * held.size, transcendentals=0),
        compiler_params=pltpu.CompilerParams(vmem_limit_bytes=61 * MIB),
        name="pack",
    )(csm, inverse, held)


def forms_kernel(rows_ref, own_ref, other_ref, e_own_ref, e_other_ref, out_ref, mat_ref):
    n_y, n_z, _, depth, width = rows_ref.shape
    half = width // 2
    core = lax.axis_index("c")
    swapped = core == 1

    for m in range(2):
        for at in range(n_y * n_z):
            y, z = at // n_z, at % n_z
            first, second = jnp.where(swapped, z, y), jnp.where(swapped, y, z)
            mat_ref[m, at * depth : (at + 1) * depth, :] = rows_ref[first, second, m]
    row = lax.broadcasted_iota(jnp.int32, (half, half), 0)
    col = lax.broadcasted_iota(jnp.int32, (half, half), 1)
    upper = col >= row
    zero = jnp.zeros((half, half), mat_ref.dtype)
    dot = functools.partial(jnp.dot, preferred_element_type=jnp.float32)
    lanes = lambda *parts: jnp.concatenate(parts, axis=1)
    tall = lambda *parts: jnp.concatenate(parts, axis=0)
    wide = lambda value: value.astype(jnp.float32)
    blocks = []
    for m in range(2):
        m00 = mat_ref[m, :half, :half]
        m11 = mat_ref[m, half:, half:]
        u01 = mat_ref[m, :half, half:]
        l10 = mat_ref[m, half:, :half]
        u00, l00 = jnp.where(upper, m00, zero), jnp.where(upper, zero, m00)
        u11, l11 = jnp.where(upper, m11, zero), jnp.where(upper, zero, m11)
        blocks.append(
            (lanes(u00, u01, -l00), lanes(l00, u00, u01), lanes(u11, -l10, -l11), lanes(l10, l11, u11))
        )
    stacked = [tall(*pair) for pair in zip(*blocks)]
    singles, peaks = [], [None, None]
    for wave_ref, energy_ref in ((own_ref, e_own_ref), (other_ref, e_other_ref)):
        r0, r1 = wave_ref[0, :half], wave_ref[0, half:]
        i0, i1 = wave_ref[1, :half], wave_ref[1, half:]
        totals = [None, None]
        for left, right, times in zip(
            stacked,
            (tall(r0, r1, i0), tall(r0, i0, i1), tall(r1, i0, i1), tall(r0, r1, i1)),
            (r0, i0, r1, i1),
        ):
            image = dot(left, right)
            times = wide(times)
            for m in range(2):
                part = jnp.sum(image[m * half : (m + 1) * half] * times, axis=0)
                totals[m] = part if totals[m] is None else totals[m] + part
        energy = energy_ref[...]
        power, quad = 2.0 * totals[0][None], 2.0 * totals[1][None]
        single = (power / energy, energy / quad)
        singles.append(single)
        for m in range(2):
            top = jnp.max(single[m], axis=1, keepdims=True)
            peaks[m] = top if peaks[m] is None else jnp.maximum(peaks[m], top)
    part_of = role()
    lane = lax.broadcasted_iota(jnp.int32, (1, 128), 1)
    at = ((lax.axis_index("x") * 2 + core) * 2 + part_of) * 2
    mark = jnp.where(lane == at, peaks[0], jnp.where(lane == at + 1, peaks[1], -jnp.inf))
    n_f = out_ref.shape[0] // 4
    share = own_ref.shape[2] // n_f
    for f in range(n_f):
        own, other = (lanes(*(p[:, f * share : (f + 1) * share] for p in single)) for single in singles)
        for py in range(2):
            for pz in range(2):
                mine = jnp.where(core == 0, pz, py) == part_of
                out_ref[(py * 2 + pz) * n_f + f] = lanes(jnp.where(mine, own, other), mark)


def fan_kernel(near_ref, out_hbm, sems):
    sends = [pltpu.make_async_copy(near_ref, out_hbm.at[to], sems.at[to]) for to in range(out_hbm.shape[0])]
    for copy in sends:
        copy.start()
    for copy in sends:
        copy.wait()


def fan(near, n_y):
    return pl.pallas_call(
        fan_kernel,
        out_shape=jax.ShapeDtypeStruct((n_y, *near.shape), near.dtype),
        in_specs=[pl.BlockSpec(memory_space=pltpu.VMEM)],
        out_specs=pl.BlockSpec(memory_space=pltpu.HBM),
        scratch_shapes=[pltpu.SemaphoreType.DMA((n_y,))],
        cost_estimate=pl.CostEstimate(flops=0, bytes_accessed=10 * near.size, transcendentals=0),
        compiler_params=pltpu.CompilerParams(vmem_limit_bytes=4 * MIB),
        name="fan",
    )(near)


def peaks_kernel(parts_ref, out_ref):
    width = out_ref.shape[2]
    top = parts_ref[0, :, width:]
    for source in range(1, parts_ref.shape[0]):
        top = jnp.maximum(top, parts_ref[source, :, width:])
    for to in range(out_ref.shape[0]):
        out_ref[to] = top


def total_kernel(count, parts_ref, tops_ref, first_ref, second_ref):
    odd_y, odd_z = lax.axis_index("yl") == 1, lax.axis_index("zl") == 1
    n_f = parts_ref.shape[0] // 4
    width = tops_ref.shape[2]
    share = width // 2
    top = tops_ref[0]
    for source in range(1, tops_ref.shape[0]):
        top = jnp.maximum(top, tops_ref[source])
    lane = lax.broadcasted_iota(jnp.int32, (1, width), 1)
    total = jnp.zeros((1, width), jnp.float32)
    for f in range(n_f):
        for part_of in range(2):
            low = part_of * n_f + f if f % 2 == 0 else part_of * 2 * n_f + f
            high = low + (2 * n_f if f % 2 == 0 else n_f)
            odd = odd_y if f % 2 == 0 else odd_z
            part = jnp.where(odd, parts_ref[high, :, :width], parts_ref[low, :, :width])
            at = (f * 2 + part_of) * 2
            total += part / jnp.where(lane < share, top[:, at : at + 1], top[:, at + 1 : at + 2])
    total = total * (1.0 / count)
    first_ref[...] = total[:, :share]
    second_ref[...] = total[:, share:]


def kernel_call(kernel, outs, operands, scratch=(), limit=4 * MIB, flops=0, dtype=jnp.float32):
    vmem = pl.BlockSpec(memory_space=pltpu.VMEM)
    cost = pl.CostEstimate(flops=flops, bytes_accessed=sum(a.size for a in operands), transcendentals=0)
    return pl.pallas_call(
        kernel,
        out_shape=tuple(jax.ShapeDtypeStruct(s, dtype) for s in outs),
        in_specs=[vmem] * len(operands),
        out_specs=[vmem] * len(outs),
        scratch_shapes=list(scratch),
        cost_estimate=cost,
        compiler_params=pltpu.CompilerParams(vmem_limit_bytes=limit),
    )(*operands)


def body(shape, replicas, csm, inverse):
    n_y, n_z, n_x, n_c = shape
    bins, points, _, width = replicas.shape
    natural = Layout(major_to_minor=(0, 1, 2))
    rows, given = pack(n_z, csm, inverse, replicas)
    got = lax.ppermute(with_layout_constraint(given, natural), ALL, partners(shape))
    got = with_layout_constraint(got, natural)
    kept = lax.dynamic_index_in_dim(replicas, role(), 0, keepdims=False)

    near = lax.all_to_all(rows, ALL, 0, 0, axis_index_groups=lines(shape, True), tiled=True)
    both = lax.all_to_all(fan(near, n_y), ALL, 0, 0, axis_index_groups=lines(shape, False), tiled=True)

    waves, energies = [], []
    for held in (kept, got):
        waves.append(jnp.transpose(held, (1, 2, 0)))
        wide = held.astype(jnp.float32)
        energies.append((jnp.sum(wide * wide, axis=(1, 2)) + 1e-06)[None])
    n_f = n_x * n_c
    share = points // n_f
    (parts,) = kernel_call(
        forms_kernel,
        ((4 * n_f, 1, 2 * share + 128),),
        (both, *waves, *energies),
        scratch=[pltpu.VMEM((2, width, width), jnp.bfloat16)],
        limit=24 * MIB,
        flops=2 * 2 * 12 * 2 * (width // 2) ** 2 * points,
    )
    parts = lax.all_to_all(parts, ("yl", "zl", "x", "c"), 0, 0, tiled=True)
    (tops,) = kernel_call(peaks_kernel, ((n_y * n_z // 4, 1, 128),), (parts,))
    tops = lax.all_to_all(tops, ("yh", "zh"), 0, 0, tiled=True)
    total = functools.partial(total_kernel, bins * n_f)
    first, second = kernel_call(total, ((1, share), (1, share)), (parts, tops))
    return first[0], second[0]


def solution(mesh):
    side = round(mesh.shape["grid"] ** 0.5)
    shape = (side, side, mesh.shape["freq"] // 2, 2)
    fine = Mesh(mesh.devices.reshape(side // 2, 2, side // 2, 2, *shape[2:]), ALL)
    grid, freq = ALL[:4], ALL[4:]
    in_specs = (P(freq, grid, None, None), P(freq, None, grid, None), P(freq, None, grid, None))
    out_specs = (P(ALL), P(ALL))

    def run(*inputs):
        return body(shape, *inputs)

    return jax.shard_map(run, mesh=fine, in_specs=in_specs, out_specs=out_specs, check_vma=False)
```

```python
import functools

import jax
import jax.numpy as jnp
import numpy as np
from jax import lax
from jax.experimental import pallas as pl
from jax.experimental.layout import Layout, with_layout_constraint
from jax.experimental.pallas import tpu as pltpu
from jax.sharding import Mesh
from jax.sharding import PartitionSpec as P

ALL = ("yh", "yl", "zh", "zl", "x", "c")
MIB = 1 << 20


def device_ids(shape):
    return np.arange(np.prod(shape)).reshape(shape)


def lines(shape, first):
    ids = device_ids(shape)
    by_y = np.moveaxis(ids, 0, -1)
    by_z = np.moveaxis(ids, 1, -1)
    pair = (by_z, by_y) if first else (by_y, by_z)
    picked = [part[..., core, :].reshape(-1, part.shape[-1]) for core, part in enumerate(pair)]
    return np.concatenate(picked, axis=0).tolist()


def partners(shape):
    ids = device_ids(shape)
    pairs = []
    for core in range(shape[3]):
        plane = ids[..., core]
        other = plane[np.arange(shape[0]) ^ 1] if core == 0 else plane[:, np.arange(shape[1]) ^ 1]
        pairs += zip(plane.ravel().tolist(), other.ravel().tolist())
    return pairs


def role():
    return jnp.where(lax.axis_index("c") == 0, lax.axis_index("yl"), lax.axis_index("zl"))


def pack_kernel(n_z, csm_hbm, inverse_hbm, rows_hbm, matrices, packed, sems):
    bins, _, depth, width = csm_hbm.shape
    to_all = rows_hbm.shape[0]
    reads = [pltpu.make_async_copy(ref, matrices.at[k], sems.at[k]) for k, ref in enumerate((csm_hbm, inverse_hbm))]
    sends = [pltpu.make_async_copy(packed, rows_hbm.at[to], sems.at[2 + to]) for to in range(to_all)]
    for copy in reads:
        copy.start()
    y = lax.axis_index("yh") * 2 + lax.axis_index("yl")
    z = lax.axis_index("zh") * 2 + lax.axis_index("zl")
    start = (y * n_z + z) * depth
    row = start + lax.broadcasted_iota(jnp.int32, (depth, width), 0)
    col = lax.broadcasted_iota(jnp.int32, (depth, width), 1)
    weight = jnp.where(col == row, 0.5, 1.0)
    for copy in reads:
        copy.wait()
    for b in range(bins):
        for m in range(2):
            real = matrices[m, b, 0].astype(jnp.float32) * weight
            imag = matrices[m, b, 1].astype(jnp.float32)
            packed[b, m] = jnp.where(col >= row, real, imag).astype(packed.dtype)
    for copy in sends:
        copy.start()
    for copy in sends:
        copy.wait()


def pack(n_z, csm, inverse):
    bins, _, depth, width = csm.shape
    hbm = pl.BlockSpec(memory_space=pltpu.HBM)
    return pl.pallas_call(
        functools.partial(pack_kernel, n_z),
        out_shape=jax.ShapeDtypeStruct((n_z, bins, 2, depth, width), csm.dtype),
        in_specs=[hbm] * 2,
        out_specs=hbm,
        scratch_shapes=[
            pltpu.VMEM((2, *csm.shape), csm.dtype),
            pltpu.VMEM((bins, 2, depth, width), csm.dtype),
            pltpu.SemaphoreType.DMA((2 + n_z,)),
        ],
        cost_estimate=pl.CostEstimate(flops=0, bytes_accessed=10 * csm.size, transcendentals=0),
        compiler_params=pltpu.CompilerParams(vmem_limit_bytes=61 * MIB),
        name="pack",
    )(csm, inverse)


def pick_kernel(flip, held_ref, out_ref, room, arrived, left):
    chosen = 1 - role() if flip else role()
    parts, size = room.shape[0], room.shape[1]
    reads = [
        pltpu.make_async_copy(held_ref.at[chosen, pl.ds(k * size, size)], room.at[k], arrived.at[k])
        for k in range(parts)
    ]
    writes = [pltpu.make_async_copy(room.at[k], out_ref.at[pl.ds(k * size, size)], left.at[k]) for k in range(parts)]
    for read in reads:
        read.start()
    for read, write in zip(reads, writes):
        read.wait()
        write.start()
    for write in writes:
        write.wait()


def pick(flip, held, parts=4):
    _, points, two, width = held.shape
    return pl.pallas_call(
        functools.partial(pick_kernel, flip),
        out_shape=jax.ShapeDtypeStruct(held.shape[1:], held.dtype),
        in_specs=[pl.BlockSpec(memory_space=pltpu.HBM)],
        out_specs=pl.BlockSpec(memory_space=pltpu.HBM),
        scratch_shapes=[
            pltpu.VMEM((parts, points // parts, two, width), held.dtype),
            pltpu.SemaphoreType.DMA((parts,)),
            pltpu.SemaphoreType.DMA((parts,)),
        ],
        cost_estimate=pl.CostEstimate(flops=0, bytes_accessed=2 * held.size, transcendentals=0),
        compiler_params=pltpu.CompilerParams(vmem_limit_bytes=61 * MIB),
    )(held)


def forms_kernel(rows_ref, own_ref, other_ref, e_own_ref, e_other_ref, out_ref, mat_ref):
    n_y, n_z, _, depth, width = rows_ref.shape
    half = width // 2
    core = lax.axis_index("c")
    swapped = core == 1

    for m in range(2):
        for at in range(n_y * n_z):
            y, z = at // n_z, at % n_z
            first, second = jnp.where(swapped, z, y), jnp.where(swapped, y, z)
            mat_ref[m, at * depth : (at + 1) * depth, :] = rows_ref[first, second, m]
    row = lax.broadcasted_iota(jnp.int32, (half, half), 0)
    col = lax.broadcasted_iota(jnp.int32, (half, half), 1)
    upper = col >= row
    zero = jnp.zeros((half, half), mat_ref.dtype)
    dot = functools.partial(jnp.dot, preferred_element_type=jnp.float32)
    lanes = lambda *parts: jnp.concatenate(parts, axis=1)
    tall = lambda *parts: jnp.concatenate(parts, axis=0)
    wide = lambda value: value.astype(jnp.float32)
    blocks = []
    for m in range(2):
        m00 = mat_ref[m, :half, :half]
        m11 = mat_ref[m, half:, half:]
        u01 = mat_ref[m, :half, half:]
        l10 = mat_ref[m, half:, :half]
        u00, l00 = jnp.where(upper, m00, zero), jnp.where(upper, zero, m00)
        u11, l11 = jnp.where(upper, m11, zero), jnp.where(upper, zero, m11)
        blocks.append(
            (lanes(u00, u01, -l00), lanes(l00, u00, u01), lanes(u11, -l10, -l11), lanes(l10, l11, u11))
        )
    stacked = [tall(*pair) for pair in zip(*blocks)]
    singles, peaks = [], [None, None]
    for wave_ref, energy_ref in ((own_ref, e_own_ref), (other_ref, e_other_ref)):
        r0, r1 = wave_ref[0, :half], wave_ref[0, half:]
        i0, i1 = wave_ref[1, :half], wave_ref[1, half:]
        totals = [None, None]
        for left, right, times in zip(
            stacked,
            (tall(r0, r1, i0), tall(r0, i0, i1), tall(r1, i0, i1), tall(r0, r1, i1)),
            (r0, i0, r1, i1),
        ):
            image = dot(left, right)
            times = wide(times)
            for m in range(2):
                part = jnp.sum(image[m * half : (m + 1) * half] * times, axis=0)
                totals[m] = part if totals[m] is None else totals[m] + part
        energy = energy_ref[...]
        power, quad = 2.0 * totals[0][None], 2.0 * totals[1][None]
        single = (power / energy, energy / quad)
        singles.append(single)
        for m in range(2):
            top = jnp.max(single[m], axis=1, keepdims=True)
            peaks[m] = top if peaks[m] is None else jnp.maximum(peaks[m], top)
    part_of = role()
    lane = lax.broadcasted_iota(jnp.int32, (1, 128), 1)
    at = ((lax.axis_index("x") * 2 + core) * 2 + part_of) * 2
    mark = jnp.where(lane == at, peaks[0], jnp.where(lane == at + 1, peaks[1], -jnp.inf))
    n_f = out_ref.shape[0] // 4
    share = own_ref.shape[2] // n_f
    for f in range(n_f):
        own, other = (lanes(*(p[:, f * share : (f + 1) * share] for p in single)) for single in singles)
        for py in range(2):
            for pz in range(2):
                mine = jnp.where(core == 0, py, pz) == part_of
                out_ref[(py * 2 + pz) * n_f + f] = lanes(jnp.where(mine, own, other), mark)


def fan_kernel(near_ref, out_hbm, sems):
    bins = near_ref.shape[1]
    sends = [
        pltpu.make_async_copy(near_ref.at[:, to % bins], out_hbm.at[to], sems.at[to]) for to in range(out_hbm.shape[0])
    ]
    for copy in sends:
        copy.start()
    for copy in sends:
        copy.wait()


def fan(near, n_y):
    n_z, _, *rest = near.shape
    return pl.pallas_call(
        fan_kernel,
        out_shape=jax.ShapeDtypeStruct((n_y, n_z, *rest), near.dtype),
        in_specs=[pl.BlockSpec(memory_space=pltpu.VMEM)],
        out_specs=pl.BlockSpec(memory_space=pltpu.HBM),
        scratch_shapes=[pltpu.SemaphoreType.DMA((n_y,))],
        cost_estimate=pl.CostEstimate(flops=0, bytes_accessed=10 * near.size, transcendentals=0),
        compiler_params=pltpu.CompilerParams(vmem_limit_bytes=4 * MIB),
        name="fan",
    )(near)


def peaks_kernel(parts_ref, out_ref):
    width = out_ref.shape[2]
    top = parts_ref[0, :, width:]
    for source in range(1, parts_ref.shape[0]):
        top = jnp.maximum(top, parts_ref[source, :, width:])
    for to in range(out_ref.shape[0]):
        out_ref[to] = top


def total_kernel(count, parts_ref, tops_ref, first_ref, second_ref):
    odd_y, odd_z = lax.axis_index("yl") == 1, lax.axis_index("zl") == 1
    n_f = parts_ref.shape[0] // 4
    width = tops_ref.shape[2]
    share = width // 2
    top = tops_ref[0]
    for source in range(1, tops_ref.shape[0]):
        top = jnp.maximum(top, tops_ref[source])
    lane = lax.broadcasted_iota(jnp.int32, (1, width), 1)
    total = jnp.zeros((1, width), jnp.float32)
    for f in range(n_f):
        for part_of in range(2):
            low = part_of * 2 * n_f + f if f % 2 == 0 else part_of * n_f + f
            high = low + (n_f if f % 2 == 0 else 2 * n_f)
            odd = odd_z if f % 2 == 0 else odd_y
            part = jnp.where(odd, parts_ref[high, :, :width], parts_ref[low, :, :width])
            at = (f * 2 + part_of) * 2
            total += part / jnp.where(lane < share, top[:, at : at + 1], top[:, at + 1 : at + 2])
    total = total * (1.0 / count)
    first_ref[...] = total[:, :share]
    second_ref[...] = total[:, share:]


def kernel_call(kernel, outs, operands, scratch=(), limit=4 * MIB, flops=0, dtype=jnp.float32):
    vmem = pl.BlockSpec(memory_space=pltpu.VMEM)
    cost = pl.CostEstimate(flops=flops, bytes_accessed=sum(a.size for a in operands), transcendentals=0)
    return pl.pallas_call(
        kernel,
        out_shape=tuple(jax.ShapeDtypeStruct(s, dtype) for s in outs),
        in_specs=[vmem] * len(operands),
        out_specs=[vmem] * len(outs),
        scratch_shapes=list(scratch),
        cost_estimate=cost,
        compiler_params=pltpu.CompilerParams(vmem_limit_bytes=limit),
    )(*operands)


def body(shape, replicas, csm, inverse):
    n_y, n_z, n_x, n_c = shape
    bins, points, _, width = replicas.shape
    natural = Layout(major_to_minor=(0, 1, 2))
    rows = pack(n_z, csm, inverse)
    given = pick(True, replicas)
    got = lax.ppermute(with_layout_constraint(given, natural), ALL, partners(shape))
    got = with_layout_constraint(got, natural)
    kept = lax.dynamic_index_in_dim(replicas, role(), 0, keepdims=False)

    near = lax.all_to_all(rows, ALL, 0, 0, axis_index_groups=lines(shape, True), tiled=True)
    both = lax.all_to_all(fan(near, n_y), ALL, 0, 0, axis_index_groups=lines(shape, False), tiled=True)

    waves, energies = [], []
    for held in (kept, got):
        waves.append(jnp.transpose(held, (1, 2, 0)))
        wide = held.astype(jnp.float32)
        energies.append((jnp.sum(wide * wide, axis=(1, 2)) + 1e-06)[None])
    n_f = n_x * n_c
    share = points // n_f
    (parts,) = kernel_call(
        forms_kernel,
        ((4 * n_f, 1, 2 * share + 128),),
        (both, *waves, *energies),
        scratch=[pltpu.VMEM((2, width, width), jnp.bfloat16)],
        limit=24 * MIB,
        flops=2 * 2 * 12 * 2 * (width // 2) ** 2 * points,
    )
    parts = lax.all_to_all(parts, ("yl", "zl", "x", "c"), 0, 0, tiled=True)
    (tops,) = kernel_call(peaks_kernel, ((n_y * n_z // 4, 1, 128),), (parts,))
    tops = lax.all_to_all(tops, ("yh", "zh"), 0, 0, tiled=True)
    total = functools.partial(total_kernel, bins * n_f)
    first, second = kernel_call(total, ((1, share), (1, share)), (parts, tops))
    return first[0], second[0]


def solution(mesh):
    side = round(mesh.shape["grid"] ** 0.5)
    shape = (side, side, mesh.shape["freq"] // 2, 2)
    fine = Mesh(mesh.devices.reshape(side // 2, 2, side // 2, 2, *shape[2:]), ALL)
    grid, freq = ALL[:4], ALL[4:]
    in_specs = (P(freq, grid, None, None), P(freq, None, grid, None), P(freq, None, grid, None))
    out_specs = (P(ALL), P(ALL))

    def run(*inputs):
        return body(shape, *inputs)

    return jax.shard_map(run, mesh=fine, in_specs=in_specs, out_specs=out_specs, check_vma=False)
```
